512 devices in a mesh: seq: 128 (over z, y, core), tp: 4 (over x).
Axes of the slice: x: 4, y: 8, z: 8, core: 2. Of those that a mesh axis runs over, the one named last changes fastest.
Arguments:
- queries: bfloat16 [12288, 4096], P('seq', 'tp'), may hold values from -8 to 8
- keys: bfloat16 [12288, 1024], P('seq', 'tp'), may hold values from -7 to 7
- values: bfloat16 [12288, 1024], P('seq', 'tp'), may hold values from -24 to 24
- router_prob: float32 [12288], P('seq'), may hold values from 0.2 to 1
- norm_gain: float32 [4096], P('tp'), may hold values from 0.25 to 1.75
- slot_pos: int32 [12288], P('seq'), may hold values from 0 to 255, as said below
- live_count: int32 [128], P('seq'), may hold values from 1 to 96, 4096 in all
Outputs:
- routed: bfloat16 [32768, 4096], P('seq', 'tp')
The draws below stay inside these ranges and needn't reach their ends.
Inputs may be any that keep to these rules, and one draw needn't show every extreme that they name: The slots of a shard that are live are its first live_count slots; the counts add up to 4096 and the largest is 96. Within each shard's 96 slots the positions are distinct and ascending; slot a of shard s stands for the token s * 256 + slot_pos[a].
All inputs are finite; a program needn't handle non-finite values.
Results may differ from the reference program's by a relative error of at most 0.007.
Values may be sent and summed in bfloat16 or wider, within the bound.
No kernel may reach another device: no remote copies, remote signals or barrier semaphores. Data moves between devices by JAX's collectives and lax.ppermute only.
A program may use at most 64 MiB of HBM per device.

```python
import math
import jax
import jax.numpy as jnp
import numpy as np
from jax import lax

H = 32
KVH = 8
HD = 128
TOK_DEV = 256
CAP = 96
SLOTS = 12288
SELECTED = 4096
TOKENS = 32768
N_SEQ = 128


def draw_queries(key, part):
    noise_key = jax.random.fold_in(key, 11)
    drawn = jnp.clip(jax.random.normal(noise_key, (SLOTS, H * HD), jnp.float32), -4.0, 4.0)
    return drawn.astype(jnp.bfloat16)


def draw_keys(key, part):
    noise_key = jax.random.fold_in(key, 12)
    drawn = jnp.clip(jax.random.normal(noise_key, (SLOTS, KVH * HD), jnp.float32), -4.0, 4.0)
    return drawn.astype(jnp.bfloat16)


def draw_values(key, part):
    noise_key = jax.random.fold_in(key, 13)
    scale_key = jax.random.fold_in(key, 31)
    head_ids = jnp.arange(KVH).astype(jnp.float32)
    ramp = 3.0 ** (head_ids / max(KVH - 1, 1))
    jitter = jnp.exp(jax.random.uniform(scale_key, (KVH,), jnp.float32, 0.0, jnp.log(2.0)))
    scales = ramp * jitter
    entries = jnp.clip(jax.random.normal(noise_key, (SLOTS, KVH * HD), jnp.float32), -4.0, 4.0)
    per_column = jnp.repeat(scales, HD)
    return (entries * per_column[None, :]).astype(jnp.bfloat16)


def draw_slot_pos(key, part):
    base_key = jax.random.fold_in(key, 14)
    shard_keys = jax.random.split(base_key, N_SEQ)

    def one_shard(shard_key):
        shuffled = jax.random.permutation(shard_key, TOK_DEV)
        return jnp.sort(shuffled[:CAP])
    return jax.vmap(one_shard)(shard_keys).reshape(SLOTS).astype(jnp.int32)


def block_scale(own_key, shape, shards, low, top_value):
    def one(dim, parts):
        draws = jax.random.uniform(jax.random.fold_in(jax.random.fold_in(own_key, 6), dim), (parts,), jnp.float32, low / len(shards), top_value / len(shards))
        return jnp.repeat(jnp.exp(draws), shape[dim] // parts).reshape((-1,) + (1,) * (len(shape) - dim - 1))

    factor_of = one(*shards[0])
    for cut in shards[1:]:
        factor_of = factor_of * one(*cut)
    return factor_of


def split_up(number_of, total, most, lean):
    loads = [(1 << 20) // math.isqrt(grade ** lean) + 1 for grade in range(2, number_of + 1)]
    surplus, given = total - most - (number_of - 1), [1] * (number_of - 1)
    while surplus > 0:
        movable = [i for i in range(number_of - 1) if given[i] < most]
        mass, remaining = sum([loads[i] for i in movable]), surplus
        for i in movable:
            addition = min(most - given[i], max(1, remaining * loads[i] // mass), surplus)
            given[i] = given[i] + addition
            surplus = surplus - addition
    return np.array([most] + given)


def uneven_parts(rng, count, total, bound, slope):
    if count == 2:
        one = jax.random.randint(rng, (), max(1, total - bound), min(bound, total - 1) + 1)
        return jnp.stack([one, total - one])
    tallies = jnp.asarray(split_up(count, total, bound, slope), jnp.int32)
    couples = (count - 1) // 2
    donor, taker = tallies[1:1 + 2 * couples:2], tallies[2:2 + 2 * couples:2]
    room = jnp.minimum(donor - 1, bound - taker)
    moved = jax.random.randint(jax.random.fold_in(rng, 1), (couples,), 0, 1 << 20) % (room + 1)
    tallies = tallies.at[1:1 + 2 * couples:2].set(donor - moved).at[2:2 + 2 * couples:2].set(taker + moved)
    return tallies[jax.random.permutation(jax.random.fold_in(rng, 2), count)]


def setup_inputs(seed: int = 0) -> dict:
    arg_keys = jax.random.split(jax.random.key(seed), 8)
    queries = draw_queries(jax.random.fold_in(arg_keys[7], 71), 0)
    keys = draw_keys(jax.random.fold_in(arg_keys[7], 71), 0)
    values = draw_values(jax.random.fold_in(arg_keys[7], 71), 0)
    router_prob = jnp.clip(0.2 + 0.8 * jax.random.uniform(arg_keys[3], (SLOTS,), jnp.float32) ** block_scale(arg_keys[3], (SLOTS,), ((0, 128),), -0.2, 0.2), 0.2, 1.0)
    norm_gain = jnp.clip(1.0 + 0.15 * jax.random.normal(arg_keys[4], (H * HD,), jnp.float32), 0.25, 1.75)
    slot_pos = draw_slot_pos(jax.random.fold_in(arg_keys[7], 71), 0)
    live_count = uneven_parts(arg_keys[6], N_SEQ, SELECTED, CAP, 2).astype(jnp.int32)
    return {"queries": queries, "keys": keys, "values": values, "router_prob": router_prob, "norm_gain": norm_gain, "slot_pos": slot_pos, "live_count": live_count}


def reference(queries, keys, values, router_prob, norm_gain, slot_pos, live_count):
    group_size = H // KVH
    limits = jnp.cumsum(live_count).astype(jnp.int32)
    starts = (limits - live_count).astype(jnp.int32)
    numbers = jnp.arange(SELECTED, dtype=jnp.int32)
    shard_of = lax.optimization_barrier(jnp.sum((limits[None, :] <= numbers[:, None]).astype(jnp.int32), axis=1)).astype(jnp.int32)
    slot_of = (numbers - starts[shard_of]).astype(jnp.int32)
    flat_index = (shard_of * CAP + slot_of).astype(jnp.int32)
    dense_queries = queries[flat_index].astype(jnp.float32)
    dense_keys = keys[flat_index].astype(jnp.float32)
    dense_values = values[flat_index]
    causal = numbers[:, None] >= numbers[None, :]
    score_scale = 1.0 / math.sqrt(HD)

    def one_head(head_number):
        kv_group = head_number // group_size
        query_head = lax.dynamic_slice_in_dim(dense_queries, head_number * HD, HD, 1)
        key_head = lax.dynamic_slice_in_dim(dense_keys, kv_group * HD, HD, 1)
        value_head = lax.dynamic_slice_in_dim(dense_values, kv_group * HD, HD, 1)
        scores = jnp.dot(query_head, key_head.T, precision=lax.Precision.HIGHEST) * score_scale
        scores = jnp.where(causal, scores, -jnp.inf)
        highest = lax.optimization_barrier(jnp.max(scores, axis=1, keepdims=True))
        weights = jnp.where(causal, jnp.exp(scores - highest), 0.0)
        totals = lax.optimization_barrier(jnp.sum(weights, axis=1, keepdims=True))
        summed = jnp.dot(weights.astype(jnp.bfloat16), value_head, preferred_element_type=jnp.float32)
        return (summed / totals).astype(jnp.bfloat16)
    heads = lax.map(one_head, jnp.arange(H, dtype=jnp.int32))
    attended = jnp.transpose(heads, (1, 0, 2)).reshape(SELECTED, H * HD)
    widened = attended.astype(jnp.float32)
    inverse = lax.rsqrt(lax.optimization_barrier(jnp.mean(widened * widened, axis=1)) + 1e-06)
    normed = router_prob[flat_index][:, None] * norm_gain[None, :] * widened * inverse[:, None]
    target_rows = (shard_of * TOK_DEV + slot_pos[flat_index]).astype(jnp.int32)
    routed = jnp.zeros((TOKENS, H * HD), jnp.bfloat16)
    return routed.at[target_rows].set(normed.astype(jnp.bfloat16))
```

```python
import math

import jax
import jax.numpy as jnp
from jax import lax
from jax.experimental import pallas as pl
from jax.experimental.pallas import tpu as pltpu
from jax.sharding import PartitionSpec as P

H = 32
HD = 128
TOK_DEV = 256
CAP = 96
SELECTED = 4096
N_SEQ = 128
LOCAL_HEADS = 8
LOCAL_GROUPS = 2
GROUP = 4
KV_COLS = 512
PAYLOAD = CAP + 8
UNIT = 16
BLOCK = 512
TAIL = 640
ROWS = GROUP * CAP
PACKED = SELECTED + N_SEQ * (UNIT - 1)
BUFFER = -(-PACKED // UNIT) * UNIT + TAIL
EPSILON = 1e-06
LOWEST = -1e30
SCALE = math.log2(math.e) / math.sqrt(HD)


def attend_kernel(counts_ref, me_ref, q_ref, kv_ref, out_ref, sq_ref, buf, flags, q_all, m_ref, acc_ref, sem):
    me = me_ref[0]
    flags[...] = jnp.ones_like(flags)

    def bring(s, at):
        n = counts_ref[s]
        size = pl.multiple_of((n + (UNIT - 1)) // UNIT * UNIT, UNIT)
        at = pl.multiple_of(at, UNIT)
        pltpu.make_async_copy(
            kv_ref.at[s, pl.ds(0, size), :], buf.at[pl.ds(at, size), :], sem
        ).start()
        last = pl.multiple_of(at + size - UNIT, UNIT)
        row = lax.broadcasted_iota(jnp.int32, (UNIT, HD), 0)
        alive = jnp.where(row < n - (size - UNIT), 1.0, 0.0)
        flags[pl.ds(last, UNIT), :] = alive.astype(jnp.bfloat16)
        return at + size

    mine = lax.fori_loop(0, me, bring, jnp.int32(0))
    end = pl.multiple_of(bring(me, mine), UNIT)
    for k in range(TAIL // UNIT):
        buf[pl.ds(pl.multiple_of(end + k * UNIT, UNIT), UNIT), :] = jnp.zeros((UNIT, KV_COLS), jnp.bfloat16)
    for g in range(LOCAL_GROUPS):
        for h in range(GROUP):
            at = (g * GROUP + h) * HD
            q_all[g, h * CAP : (h + 1) * CAP, :] = q_ref[:, at : at + HD]
    m_ref[...] = jnp.full_like(m_ref, LOWEST)
    acc_ref[...] = jnp.zeros_like(acc_ref)
    pltpu.make_async_copy(buf.at[pl.ds(0, end), :], buf.at[pl.ds(0, end), :], sem).wait()

    def fold(start, width, masked):
        for g in range(LOCAL_GROUPS):
            keys = buf[pl.ds(start, width), g * HD : (g + 1) * HD]
            values = buf[pl.ds(start, width), (LOCAL_GROUPS + g) * HD : (LOCAL_GROUPS + g + 1) * HD]
            both = jnp.concatenate([values, flags[pl.ds(start, width), :]], axis=1)
            scores = lax.dot_general(
                q_all[g], keys, (((1,), (1,)), ((), ())), preferred_element_type=jnp.float32
            )
            if masked:
                col = lax.broadcasted_iota(jnp.int32, (1, CAP, width), 2)
                row = lax.broadcasted_iota(jnp.int32, (1, CAP, width), 1)
                visible = col - row <= mine - start
                scores = jnp.where(visible, scores.reshape(GROUP, CAP, width), LOWEST)
                scores = scores.reshape(ROWS, width)
            old = m_ref[g]
            new = jnp.maximum(old, jnp.max(scores, axis=1, keepdims=True))
            weights = jnp.exp2((scores - new[:, :1]) * SCALE).astype(jnp.bfloat16)
            factor = jnp.exp2((old - new) * SCALE)
            m_ref[g] = new
            update = jnp.dot(weights, both, preferred_element_type=jnp.float32)
            acc_ref[g] = acc_ref[g] * jnp.concatenate([factor, factor], axis=1) + update

    blocks = mine // BLOCK

    def full(i, _):
        fold(pl.multiple_of(i * BLOCK, BLOCK), BLOCK, False)
        return 0

    lax.fori_loop(0, blocks, full, 0)
    fold(pl.multiple_of(blocks * BLOCK, BLOCK), TAIL, True)
    squares = jnp.zeros((CAP, HD), jnp.float32)
    for g in range(LOCAL_GROUPS):
        acc = acc_ref[g]
        attended = (acc[:, :HD] / acc[:, HD:]).astype(jnp.bfloat16)
        for h in range(GROUP):
            at = (g * GROUP + h) * HD
            piece = attended[h * CAP : (h + 1) * CAP]
            out_ref[:, at : at + HD] = piece
            wide = piece.astype(jnp.float32)
            squares = squares + wide * wide
    square = jnp.concatenate([squares, jnp.zeros((HD - CAP, HD), jnp.float32)], axis=0)
    sq_ref[...] = jnp.sum(jnp.transpose(square), axis=0, keepdims=True)


def attend(counts, me, queries, gathered):
    return pl.pallas_call(
        attend_kernel,
        grid_spec=pltpu.PrefetchScalarGridSpec(
            num_scalar_prefetch=2,
            grid=(),
            in_specs=[
                pl.BlockSpec(memory_space=pltpu.VMEM),
                pl.BlockSpec(memory_space=pl.ANY),
            ],
            out_specs=[
                pl.BlockSpec(memory_space=pltpu.VMEM),
                pl.BlockSpec(memory_space=pltpu.VMEM),
            ],
            scratch_shapes=[
                pltpu.VMEM((BUFFER, KV_COLS), jnp.bfloat16),
                pltpu.VMEM((BUFFER, HD), jnp.bfloat16),
                pltpu.VMEM((LOCAL_GROUPS, ROWS, HD), jnp.bfloat16),
                pltpu.VMEM((LOCAL_GROUPS, ROWS, HD), jnp.float32),
                pltpu.VMEM((LOCAL_GROUPS, ROWS, 2 * HD), jnp.float32),
                pltpu.SemaphoreType.DMA(()),
            ],
        ),
        out_shape=[
            jax.ShapeDtypeStruct((CAP, LOCAL_HEADS * HD), jnp.bfloat16),
            jax.ShapeDtypeStruct((1, HD), jnp.float32),
        ],
        name="attend",
    )(counts, me, queries, gathered)


def local(queries, keys, values, router_prob, norm_gain, slot_pos, live_count):
    slot_index = jnp.arange(CAP, dtype=jnp.int32)
    alive = slot_index < live_count[0]
    sent_keys = jnp.where(alive[:, None], keys, keys[:1])
    sent_values = jnp.where(alive[:, None], values, jnp.zeros_like(values))
    count_rows = jnp.broadcast_to(live_count.astype(jnp.bfloat16)[None, :], (PAYLOAD - CAP, KV_COLS))
    payload = jnp.concatenate([jnp.concatenate([sent_keys, sent_values], axis=1), count_rows], axis=0)
    gathered = lax.all_gather(payload, "seq", axis=0)
    counts = gathered[:, CAP, 0].astype(jnp.int32)
    me = lax.axis_index("seq").astype(jnp.int32).reshape(1)
    attended, squares = attend(counts, me, queries, gathered)
    total_squares = lax.psum(squares, "tp")[0, :CAP]
    inverse = lax.rsqrt(total_squares / (H * HD) + EPSILON)
    widened = attended.astype(jnp.float32)
    normed = (router_prob[:, None] * norm_gain[None, :] * widened * inverse[:, None]).astype(
        jnp.bfloat16
    )
    placer = (
        (jnp.arange(TOK_DEV, dtype=jnp.int32)[:, None] == slot_pos[None, :]) & alive[None, :]
    ).astype(jnp.bfloat16)
    return jnp.dot(placer, normed, preferred_element_type=jnp.float32).astype(jnp.bfloat16)


def solution(mesh):
    in_specs = (
        P("seq", "tp"),
        P("seq", "tp"),
        P("seq", "tp"),
        P("seq"),
        P("tp"),
        P("seq"),
        P("seq"),
    )
    out_specs = P("seq", "tp")
    return jax.shard_map(local, mesh=mesh, in_specs=in_specs, out_specs=out_specs, check_vma=False)
```
